128 devices in a mesh: row: 16 (over z, y), col: 8 (over x, core).
Axes of the slice: x: 4, y: 4, z: 4, core: 2. Of those that a mesh axis runs over, the one named last changes fastest.
Arguments:
- act_quant: bfloat16 [1024, 8192], P('row', 'col'), may hold values from -127 to 127, as said below
- act_scale: float32 [1024], replicated, may hold values from 0.004 to 0.04
- gate_up_quant: bfloat16 [2, 8192, 29568], P(None, 'col', 'row'), may hold values from -127 to 127, as said below
- gate_up_scale: float32 [2, 29568], P(None, 'row'), may hold values from 5e-05 to 0.0005
- down_quant: bfloat16 [29568, 8192], P('row', 'col'), may hold values from -127 to 127, as said below
- down_scale: float32 [8192], P('col'), may hold values from 3e-05 to 0.0003
Outputs:
- mixed_out: bfloat16 [1024, 8192], P('row', 'col')
The draws below stay inside these ranges and needn't reach their ends.
Inputs may be any that keep to these rules, and one draw needn't show every extreme that they name: `act_quant`: whole numbers. `gate_up_quant`: whole numbers. `down_quant`: whole numbers.
All inputs are finite; a program needn't handle non-finite values.
Results may differ from the reference program's by a relative error of at most 0.005.
Values may be sent and summed in bfloat16 or wider, within the bound.
A program may use at most 128 MiB of HBM per device.

```python
import math
import jax
import jax.numpy as jnp

D = 8192
FF = 29568
TOK = 1024


def integer_levels(key, shape_dims):
    levels = jax.random.randint(key, shape_dims, -127, 128)
    return levels.astype(jnp.float32).astype(jnp.bfloat16)


def draw_act_quant(key, part):
    return integer_levels(jax.random.fold_in(key, 11), (TOK, D))


def draw_gate_up_quant(key, part):
    return integer_levels(jax.random.fold_in(key, 22), (2, D, FF))


def draw_down_quant(key, part):
    return integer_levels(jax.random.fold_in(key, 33), (FF, D))


def steps_of(rng, shape, pieces, least, top_value):
    level = 1.0
    for axis_at, parts in pieces:
        heights = jax.random.uniform(jax.random.fold_in(jax.random.fold_in(rng, 6), axis_at), (parts,), jnp.float32, least / len(pieces), top_value / len(pieces))
        level = level * jnp.repeat(jnp.exp(heights), shape[axis_at] // parts).reshape((-1,) + (1,) * (len(shape) - 1 - axis_at))
    return level


def setup_inputs(seed: int = 0) -> dict:
    keys = jax.random.split(jax.random.key(seed), 7)
    return {
        "act_quant": draw_act_quant(jax.random.fold_in(keys[6], 71), 0),
        "act_scale": jnp.clip(jnp.exp(jax.random.uniform(keys[1], (TOK,), jnp.float32, math.log(0.004), math.log(0.04))), 0.004, 0.04),
        "gate_up_quant": draw_gate_up_quant(jax.random.fold_in(keys[6], 71), 0),
        "gate_up_scale": jnp.clip(jnp.exp(math.log(0.0005) - 2.3025852 * jax.random.uniform(keys[3], (2, FF), jnp.float32) ** steps_of(keys[3], (2, FF), ((1, 16),), -0.2, 0.2)), 4.999999873689376e-05, 0.0005),
        "down_quant": draw_down_quant(jax.random.fold_in(keys[6], 71), 0),
        "down_scale": jnp.clip(jnp.exp(math.log(0.0003) - 2.3025852 * jax.random.uniform(keys[5], (D,), jnp.float32) ** steps_of(keys[5], (D,), ((0, 8),), -0.2, 0.2)), 2.9999999242136255e-05, 0.0003),
    }


def reference(act_quant, act_scale, gate_up_quant, gate_up_scale, down_quant, down_scale):
    gate_acc = jnp.dot(act_quant, gate_up_quant[0], preferred_element_type=jnp.float32)
    up_acc = jnp.dot(act_quant, gate_up_quant[1], preferred_element_type=jnp.float32)
    gate_val = gate_acc * act_scale[:, None] * gate_up_scale[0][None, :]
    up_val = up_acc * act_scale[:, None] * gate_up_scale[1][None, :]
    hidden = (jax.nn.silu(gate_val) * up_val).astype(jnp.bfloat16)
    out_acc = jnp.dot(hidden, down_quant, preferred_element_type=jnp.float32)
    return (out_acc * down_scale[None, :]).astype(jnp.bfloat16)
```

```python
import jax
import jax.numpy as jnp
from jax import lax
from jax.experimental import pallas as pl
from jax.experimental.pallas import tpu as pltpu
from jax.sharding import PartitionSpec as P

MESH = pl.DeviceIdType.MESH
CHUNKS = 4
F32 = jnp.float32
BF16 = jnp.bfloat16
OFFSETS = [(a, b) for a in range(4) for b in range(4) if a or b]
PIECES = ((0, 1024, 0), (1024, 768, 0), (1792, 1024, 1), (2816, 880, 1))
ORDER = (
    "A00 A10 A20 A30", "B00 B10 B20 B30", "A01 A11 C00 C10", "A21 A31 C20 C30",
    "B01 B11 B21 B31", "A02 A12 A22 A32", "D.0 C01 C11", "C21 C31 B02",
    "B12 B22 B32 E.0", "A03 A13 A23 A33", "D.1 e.0 C02 C12", "C22 C32 B03",
    "B13 B23 B33 E.1", "F.0 D.2 C03 C13", "C23 C33 e.1", "E.2 F.1 J.0 D.3",
    "e.2 F.2 E.3 J.1", "e.3 F.3 J.2 J.3",
)


def kernel(
    act_hbm, act_scale, gate_up_hbm, gate_up_scale, down_hbm, down_scale, out,
    act, w, dn, acc, pair, first, direct, merge, own, first_in, left_in, right_in,
    hid, o_send, o_recv, scale, load_sem, send_sem, recv_sem,
):
    n, rows, tok, width = act.shape
    feats = hid.shape[3]
    row, col = lax.axis_index("row"), lax.axis_index("col")
    z, y, x, core = row // 4, row % 4, col // 2, col % 2
    x1, x2, x3 = (x + 1) % 4, (x + 2) % 4, (x + 3) % 4
    xp, xm = (row, x1 * 2 + core), (row, x3 * 2 + core)
    mate = (row, x * 2 + 1 - core)
    peers = [((z + a) % 4 * 4 + (y + b) % 4, col) for a, b in OFFSETS]

    def load(src, dst, index):
        copy = pltpu.make_async_copy(src, dst, load_sem.at[index])
        copy.start()
        return copy

    own_loads = [
        load(act_hbm.at[pl.ds(tok * i, tok)], act.at[i, row], i) for i in range(n)
    ]
    w_loads = [
        load(gate_up_hbm.at[pl.ds(s, m)], w.at[pl.ds(s, m)], n + p)
        for p, (s, m, _) in enumerate(PIECES)
    ]
    dn_load = load(down_hbm, dn, n + len(PIECES))

    names = {}
    copies = [{} for _ in range(n)]

    def send(i, name, src, dst, device):
        index = names.setdefault(name, len(names))
        copy = pltpu.make_async_remote_copy(
            src_ref=src, dst_ref=dst, send_sem=send_sem.at[i, index],
            recv_sem=recv_sem.at[i, index], device_id=device, device_id_type=MESH,
        )
        copy.start()
        copies[i][name] = copy

    def got(i, *which):
        for name in which:
            copies[i][name].wait_recv()

    barrier = pltpu.get_barrier_semaphore()
    near = [xp, xm, mate, *peers]
    for device in near:
        pl.semaphore_signal(barrier, inc=1, device_id=device, device_id_type=MESH)

    lane = lax.broadcasted_iota(jnp.int32, (128, 128), 1)
    line = lax.broadcasted_iota(jnp.int32, (128, 128), 0)
    mine = jnp.broadcast_to(act_scale[pl.ds(col, 1), :], (128, 128))
    column = jnp.sum(jnp.where(lane == line, mine, 0.0), axis=1, keepdims=True)
    scale[...] = jnp.broadcast_to(column, (128, 128))

    pl.semaphore_wait(barrier, len(near))

    for i in range(n):
        own_loads[i].wait()
        for q, peer in enumerate(peers):
            send(i, f"a{q}", act.at[i, row], act.at[i, row], peer)

    def stage_a(i, p):
        start, size, _ = PIECES[p]
        cols = pl.ds(start, size)
        if p == 0:
            got(i, *[f"a{q}" for q in range(len(peers))])
            if i >= 2:
                for q in range(len(PIECES)):
                    copies[i - 2].pop(f"p{q}").wait_send()
        if i == 0:
            w_loads[p].wait()
        part = lax.dot_general(
            act[i].reshape(rows * tok, width), w[cols, :], (((1,), (1,)), ((), ())),
            preferred_element_type=F32,
        )
        s = i % 2
        acc[s, :, :, :, cols] = part.reshape(4, 2, 2 * tok, size)
        send(i, f"p{p}", acc.at[s, :, 1 - core, :, cols], pair.at[i, :, :, cols], mate)

    def stage_b(i, p):
        start, size, side = PIECES[p]
        cols = pl.ds(start, size)
        s = i % 2

        def both(d):
            return acc[s, d, core, :, cols] + pair[i, d, :, cols]

        got(i, f"p{p}")
        near_dev, far_dev = (xm, xp) if side == 0 else (xp, xm)
        near_x, far_x = (x3, x1) if side == 0 else (x1, x3)
        landing = right_in if side == 0 else left_in
        first[i, :, cols] = both(x2).astype(BF16)
        send(i, f"s{p}", first.at[i, :, cols], first_in.at[i, :, cols], far_dev)
        direct[i, :, cols] = both(near_x).astype(BF16)
        send(i, f"d{p}", direct.at[i, :, cols], landing.at[i, :, cols], near_dev)
        merge[i, :, cols] = both(far_x)
        own[i, :, cols] = both(x)

    def stage_c(i, p):
        start, size, side = PIECES[p]
        cols = pl.ds(start, size)
        far_dev, landing = (xp, left_in) if side == 0 else (xm, right_in)
        got(i, f"s{p}")
        copies[i].pop(f"s{p}").wait_send()
        first[i, :, cols] = (merge[i, :, cols] + first_in[i, :, cols].astype(F32)).astype(BF16)
        send(i, f"m{p}", first.at[i, :, cols], landing.at[i, :, cols], far_dev)

    def pass_on(i, name, block, device, start=0, size=None):
        part = hid.at[i, block, pl.ds(start, size or 2 * tok)]
        send(i, name, part, part, device)

    def stage_d(i):
        got(i, *[kind + str(p) for kind in "dm" for p in range(len(PIECES))])
        total = own[i] + left_in[i].astype(F32) + right_in[i].astype(F32)
        token = jnp.concatenate(
            [scale[pl.ds(tok * i, tok), 0:1], scale[pl.ds(64 + tok * i, tok), 0:1]], axis=0
        )
        gate = total[:, :feats] * token * gate_up_scale[0:1, :]
        up = total[:, feats:] * token * gate_up_scale[1:2, :]
        hid[i, col] = (gate / (1.0 + jnp.exp(-gate)) * up).astype(BF16)
        pass_on(i, "hp", col, xp)
        pass_on(i, "hm", col, xm)
        pass_on(i, "hc", col, mate)

    def stage_e(i):
        left, right = x3 * 2 + core, x1 * 2 + core
        got(i, "hp")
        pass_on(i, "hfp", left, xp, 0, tok)
        pass_on(i, "hcl", left, mate)
        got(i, "hm")
        pass_on(i, "hfm", right, xm, tok, tok)
        pass_on(i, "hcr", right, mate)

    def stage_e2(i):
        got(i, "hfp", "hfm")
        pass_on(i, "hcf", x2 * 2 + core, mate)

    def stage_f(i):
        got(i, "hc", "hcl", "hcr", "hcf")
        if i == 0:
            dn_load.wait()
        for j in range(2):
            cols = pl.ds(j * width // 2, width // 2)
            part = jnp.dot(
                hid[i].reshape(rows * tok, feats), dn[:, cols], preferred_element_type=F32
            )
            part = (part * down_scale[:, cols]).astype(BF16)
            o_send[i, :, :, cols] = part.reshape(rows, tok, width // 2)
        for q, peer in enumerate(peers):
            send(i, f"o{q}", o_send.at[i, peer[0]], o_recv.at[i, q], peer)

    def stage_j(i):
        got(i, *[f"o{q}" for q in range(len(peers))])
        total = o_send[i, row].astype(F32)
        for q in range(len(peers)):
            total = total + o_recv[i, q].astype(F32)
        out[pl.ds(tok * i, tok), :] = total.astype(BF16)

    stages = {
        "A": stage_a, "B": stage_b, "C": stage_c, "D": stage_d, "E": stage_e,
        "e": stage_e2, "F": stage_f, "J": stage_j,
    }
    for words in ORDER:
        for word in words.split():
            name, piece, chunk = word
            if piece == ".":
                stages[name](int(chunk))
            else:
                stages[name](int(chunk), int(piece))
    for i in range(n):
        for copy in copies[i].values():
            copy.wait_send()


def body(act_quant, act_scale, gate_up_quant, gate_up_scale, down_quant, down_scale):
    local_rows, width = act_quant.shape
    feats = gate_up_quant.shape[2]
    rows = lax.axis_size("row")
    n, tok = CHUNKS, local_rows // CHUNKS
    block = 2 * tok
    any_spec = pl.BlockSpec(memory_space=pl.ANY)
    vmem_spec = pl.BlockSpec(memory_space=pltpu.VMEM)
    vmem = pltpu.VMEM
    return pl.pallas_call(
        kernel,
        out_shape=jax.ShapeDtypeStruct((local_rows, width), BF16),
        in_specs=[any_spec, vmem_spec, any_spec, vmem_spec, any_spec, vmem_spec],
        out_specs=vmem_spec,
        scratch_shapes=[
            vmem((n, rows, tok, width), BF16),
            vmem((2 * feats, width), BF16),
            vmem((feats, width), BF16),
            vmem((2, 4, 2, block, 2 * feats), F32),
            vmem((n, 4, block, 2 * feats), F32),
            vmem((n, block, 2 * feats), BF16),
            vmem((n, block, 2 * feats), BF16),
            vmem((n, block, 2 * feats), F32),
            vmem((n, block, 2 * feats), F32),
            vmem((n, block, 2 * feats), BF16),
            vmem((n, block, 2 * feats), BF16),
            vmem((n, block, 2 * feats), BF16),
            vmem((n, 8, block, feats), BF16),
            vmem((n, rows, tok, width), BF16),
            vmem((n, rows - 1, tok, width), BF16),
            vmem((128, 128), F32),
            pltpu.SemaphoreType.DMA((n + 5,)),
            pltpu.SemaphoreType.DMA((n, 54)),
            pltpu.SemaphoreType.DMA((n, 54)),
        ],
        compiler_params=pltpu.CompilerParams(
            collective_id=0, has_side_effects=True, vmem_limit_bytes=63_000_000
        ),
        name="gated_ffn",
    )(
        act_quant, act_scale.reshape(8, 128),
        jnp.swapaxes(gate_up_quant, 1, 2).reshape(2 * feats, width), gate_up_scale,
        down_quant, down_scale.reshape(1, width),
    )


def solution(mesh):
    in_specs = (
        P("row", "col"),
        P(),
        P(None, "col", "row"),
        P(None, "row"),
        P("row", "col"),
        P("col"),
    )
    out_specs = P("row", "col")
    return jax.shard_map(body, mesh=mesh, in_specs=in_specs, out_specs=out_specs, check_vma=False)
```

```python
import jax
import jax.numpy as jnp
from jax import lax
from jax.experimental import pallas as pl
from jax.experimental.pallas import tpu as pltpu
from jax.sharding import PartitionSpec as P

MESH = pl.DeviceIdType.MESH
CHUNKS = 4
F32 = jnp.float32
BF16 = jnp.bfloat16
OFFSETS = [(a, b) for a in range(4) for b in range(4) if a or b]
PIECES = ((0, 1024, 0), (1024, 768, 0), (1792, 1024, 1), (2816, 880, 1))
UNITS = ((0, (0, 1)), (1, (0, 1)), (2, (0, 1)), (3, (0,)), (3, (1,)))
ORDER = (
    "p.0 q.0 p.1 r.0", "q.1 s.0 r.1 t.0", "A00 A10 A20 A30", "B00 B10 B20 B30",
    "s.1 g.2 t.1 A01", "A11 C00 C10 A21", "A31 C20 C30 B01", "B11 B21 B31 g.3",
    "A02 A12 A22 A32", "D.0 C01 C11 C21", "C31 B02 B12 B22", "B32 E.0 A03 A13",
    "A23 A33 D.1 C02", "C12 C22 C32 B03", "B13 B23 B33 E.1", "F.0 D.2 C03 C13",
    "C23 C33 B04 B14", "B24 B34 E.2 F.1", "D.3 C04 C14 C24", "C34 F.2 E.3 D.4",
    "J.0 F.3 E.4 J.1", "F.4 J.2 J.3 J.4",
)


def kernel(
    act_hbm, act_scale, gate_up_hbm, gate_up_scale, down_hbm, down_scale, out,
    act, w, dn, acc, pair, first, direct, merge, own, first_in, left_in, right_in,
    hid, o_send, o_recv, scale, load_sem, send_sem, recv_sem, out_sem,
):
    n, rows, tok, width = act.shape
    half = width // 2
    feats = hid.shape[4]
    row, col = lax.axis_index("row"), lax.axis_index("col")
    z, y, x, core = row // 4, row % 4, col // 2, col % 2
    x1, x2, x3 = (x + 1) % 4, (x + 2) % 4, (x + 3) % 4
    y1, y2, y3 = (y + 1) % 4, (y + 2) % 4, (y + 3) % 4
    z1, z3 = (z + 1) % 4, (z + 3) % 4
    xp, xm = (row, x1 * 2 + core), (row, x3 * 2 + core)
    yp, ym = (z * 4 + y1, col), (z * 4 + y3, col)
    zp, zm = (z1 * 4 + y, col), (z3 * 4 + y, col)
    mate = (row, x * 2 + 1 - core)
    peers = [((z + a) % 4 * 4 + (y + b) % 4, col) for a, b in OFFSETS]

    def load(src, dst, index):
        copy = pltpu.make_async_copy(src, dst, load_sem.at[index])
        copy.start()
        return copy

    own_loads = [
        load(act_hbm.at[pl.ds(tok * i, tok)], act.at[i, row], i) for i in range(n)
    ]
    w_loads = [
        load(gate_up_hbm.at[pl.ds(s, m)], w.at[pl.ds(s, m)], n + p)
        for p, (s, m, _) in enumerate(PIECES)
    ]
    dn_load = load(down_hbm, dn.at[core], n + len(PIECES))

    names, spare = {}, iter(range(176, 256))
    copies = {}

    def send(key, name, src, dst, device):
        index = names.setdefault((key, name), len(names))
        copy = pltpu.make_async_remote_copy(
            src_ref=src, dst_ref=dst, send_sem=send_sem.at[index],
            recv_sem=recv_sem.at[index],
            device_id=device, device_id_type=MESH,
        )
        copy.start()
        copies[key, name] = copy

    def got(key, *which):
        for name in which:
            copies[key, name].wait_recv()

    barrier = pltpu.get_barrier_semaphore()
    near = (xp, xm, mate, yp, ym, zp, zm)
    for device in near:
        pl.semaphore_signal(barrier, inc=1, device_id=device, device_id_type=MESH)

    lane = lax.broadcasted_iota(jnp.int32, (128, 128), 1)
    line = lax.broadcasted_iota(jnp.int32, (128, 128), 0)
    mine = jnp.broadcast_to(act_scale[pl.ds(col, 1), :], (128, 128))
    column = jnp.sum(jnp.where(lane == line, mine, 0.0), axis=1, keepdims=True)
    scale[...] = jnp.broadcast_to(column, (128, 128))

    pl.semaphore_wait(barrier, len(near))

    def r_at(zz, yy):
        return zz * 4 + yy

    def spread(i, name, block):
        send(("a", i), name + "p", act.at[i, block], act.at[i, block], zp)
        send(("a", i), name + "m", act.at[i, block], act.at[i, block], zm)

    def forward(i, name, yy):
        got(("a", i), name + "p", name + "m")
        low = act.at[i, r_at(z3, yy), :, pl.ds(0, half)]
        high = act.at[i, r_at(z1, yy), :, pl.ds(half, half)]
        send(("a", i), "f" + name + "p", low, low, zp)
        send(("a", i), "f" + name + "m", high, high, zm)

    def stage_p(i):
        own_loads[i].wait()
        send(("a", i), "y1p", act.at[i, row], act.at[i, row], yp)
        send(("a", i), "y1m", act.at[i, row], act.at[i, row], ym)
        spread(i, "za", row)

    def stage_q(i):
        got(("a", i), "y1p", "y1m")
        low = act.at[i, r_at(z, y3), :, pl.ds(0, half)]
        high = act.at[i, r_at(z, y1), :, pl.ds(half, half)]
        send(("a", i), "y2p", low, low, yp)
        send(("a", i), "y2m", high, high, ym)
        spread(i, "zb", r_at(z, y3))
        spread(i, "zc", r_at(z, y1))

    def stage_r(i):
        got(("a", i), "y2p", "y2m")
        spread(i, "zd", r_at(z, y2))
        forward(i, "za", y)

    def stage_s(i):
        forward(i, "zb", y3)
        forward(i, "zc", y1)
        forward(i, "zd", y2)
        if i == 0:
            send("dn", "", down_hbm, dn.at[core], mate)

    def stage_t(i):
        got(("a", i), *["fz" + k + d for k in "abcd" for d in "pm"])

    def stage_g(i):
        own_loads[i].wait()
        for q, peer in enumerate(peers):
            send(("a", i), f"a{q}", act.at[i, row], act.at[i, row], peer)

    def stage_a(i, p):
        start, size, _ = PIECES[p]
        cols = pl.ds(start, size)
        if p == 0:
            if (("a", i), "a0") in copies:
                got(("a", i), *[f"a{q}" for q in range(len(peers))])
            if i >= 2:
                for q in range(len(PIECES)):
                    copies.pop((("p", i - 2), q)).wait_send()
        if i == 0:
            w_loads[p].wait()
        part = lax.dot_general(
            act[i].reshape(rows * tok, width), w[cols, :], (((1,), (1,)), ((), ())),
            preferred_element_type=F32,
        )
        s = i % 2
        acc[s, :, :, :, :, cols] = part.reshape(4, 2, 2, tok, size)
        send(
            ("p", i), p, acc.at[s, :, 1 - core, :, :, cols], pair.at[i, :, :, :, cols], mate
        )

    def slots(u):
        hs = UNITS[u][1]
        return pl.ds(hs[0], len(hs))

    def stage_b(u, p):
        i, hs = UNITS[u]
        start, size, side = PIECES[p]
        cols = pl.ds(start, size)
        s, sl = i % 2, slots(u)

        def both(d):
            j = pl.ds(0, 2) if len(hs) == 2 else pl.ds((hs[0] + d) % 2, 1)
            return acc[s, d, core, j, :, cols] + pair[i, d, j, :, cols]

        if hs[0] == 0:
            got(("p", i), p)
        near_dev, far_dev = (xm, xp) if side == 0 else (xp, xm)
        near_x, far_x = (x3, x1) if side == 0 else (x1, x3)
        landing = right_in if side == 0 else left_in
        first[i, sl, :, cols] = both(x2).astype(BF16)
        send(u, f"s{p}", first.at[i, sl, :, cols], first_in.at[i, sl, :, cols], far_dev)
        direct[i, sl, :, cols] = both(near_x).astype(BF16)
        send(u, f"d{p}", direct.at[i, sl, :, cols], landing.at[i, sl, :, cols], near_dev)
        merge[i, sl, :, cols] = both(far_x)
        own[i, sl, :, cols] = both(x)

    def stage_c(u, p):
        i, sl = UNITS[u][0], slots(u)
        start, size, side = PIECES[p]
        cols = pl.ds(start, size)
        far_dev, landing = (xp, left_in) if side == 0 else (xm, right_in)
        got(u, f"s{p}")
        copies.pop((u, f"s{p}")).wait_send()
        total = merge[i, sl, :, cols] + first_in[i, sl, :, cols].astype(F32)
        first[i, sl, :, cols] = total.astype(BF16)
        send(u, f"m{p}", first.at[i, sl, :, cols], landing.at[i, sl, :, cols], far_dev)

    def pass_on(u, name, d, device, start=0, size=None):
        i, sl = UNITS[u][0], slots(u)
        part = hid.at[i, sl, d, :, pl.ds(start, size or feats)]
        send(u, name, part, part, device)

    def stage_d(u):
        i, hs = UNITS[u]
        sl = slots(u)
        got(u, *[kind + str(p) for kind in "dm" for p in range(len(PIECES))])
        total = own[i, sl] + left_in[i, sl].astype(F32) + right_in[i, sl].astype(F32)
        total = total.reshape(len(hs) * tok, 2 * feats)
        if len(hs) == 2:
            token = jnp.concatenate(
                [scale[pl.ds(tok * i, tok), 0:1], scale[pl.ds(64 + tok * i, tok), 0:1]], axis=0
            )
        else:
            begin = pl.multiple_of((hs[0] + x) % 2 * 64 + tok * i, tok)
            token = scale[pl.ds(begin, tok), 0:1]
        gate = total[:, :feats] * token * gate_up_scale[0:1, :]
        up = total[:, feats:] * token * gate_up_scale[1:2, :]
        value = (gate / (1.0 + jnp.exp(-gate)) * up).astype(BF16)
        hid[i, sl, x] = value.reshape(len(hs), tok, feats)
        pass_on(u, "hp", x, xp)
        pass_on(u, "hm", x, xm)

    split = feats // 256 * 128

    def stage_e(u):
        got(u, "hp")
        pass_on(u, "hfp", x3, xp, 0, split)
        got(u, "hm")
        pass_on(u, "hfm", x1, xm, split, feats - split)

    def is_self(a, to_y, to_core):
        return (to_y == y) & (to_core == core) if a == 0 else None

    def unless(skip, todo):
        if skip is None:
            todo()
        else:
            pl.when(jnp.logical_not(skip))(todo)

    out_sends = []

    def stage_f(u):
        i, hs = UNITS[u]
        sl = slots(u)
        got(u, "hfp", "hfm")
        if i == 0:
            dn_load.wait()
            got("dn", "")
        count = len(hs)
        for h in range(2):
            for c in range(2):
                cols = pl.ds(c * half, half)
                part = jnp.dot(
                    hid[i, sl].reshape(count * 4 * tok, feats), dn[h, :, cols],
                    preferred_element_type=F32,
                )
                o_send[i, h, sl, :, :, cols] = part.astype(BF16).reshape(count, 4, tok, half)
            for a in range(4):
                d = (z + a) % 4
                for slot in hs:
                    j = slot if count == 2 else (slot + d) % 2
                    to_y = 2 * core + j
                    skip = is_self(a, to_y, h)
                    index, device = a * 4 + y, (d * 4 + to_y, x * 2 + h)

                    def build(h=h, slot=slot, d=d, device=device, index=index, k=next(spare)):
                        return pltpu.make_async_remote_copy(
                            src_ref=o_send.at[i, h, slot, d], dst_ref=o_recv.at[i, index],
                            send_sem=send_sem.at[k], recv_sem=out_sem.at[i, index],
                            device_id=device, device_id_type=MESH,
                        )

                    unless(skip, lambda build=build: build().start())
                    out_sends.append((skip, build))

    def stage_j(u):
        i, hs = UNITS[u]
        mine = y // 2 == core
        own_slot = y % 2 if len(hs) == 2 else hs[0]

        def take():
            @pl.when(mine)
            def _():
                o_recv[i, y] = o_send[i, core, own_slot, z]

            for q in range(16):
                def wait(q=q):
                    pltpu.make_async_remote_copy(
                        src_ref=o_recv.at[i, q], dst_ref=o_recv.at[i, q],
                        send_sem=send_sem.at[0], recv_sem=out_sem.at[i, q],
                        device_id=mate, device_id_type=MESH,
                    ).wait_recv()

                unless((q == y) & mine if q < 4 else None, wait)
            total = o_recv[i, 0].astype(F32)
            for q in range(1, 16):
                total = total + o_recv[i, q].astype(F32)
            out[pl.ds(tok * i, tok), :] = (total * down_scale[...]).astype(BF16)

        if len(hs) == 2:
            take()
        else:
            pl.when((y + z) % 2 == hs[0])(take)

    stages = {
        "p": stage_p, "q": stage_q, "r": stage_r, "s": stage_s, "t": stage_t,
        "g": stage_g, "A": stage_a, "B": stage_b, "C": stage_c, "D": stage_d,
        "E": stage_e, "F": stage_f, "J": stage_j,
    }
    for words in ORDER:
        for word in words.split():
            name, piece, chunk = word
            if piece == ".":
                stages[name](int(chunk))
            else:
                stages[name](int(chunk), int(piece))
    for copy in copies.values():
        copy.wait_send()
    for skip, build in out_sends:
        unless(skip, lambda build=build: build().wait_send())


def body(act_quant, act_scale, gate_up_quant, gate_up_scale, down_quant, down_scale):
    local_rows, width = act_quant.shape
    feats = gate_up_quant.shape[2]
    rows = lax.axis_size("row")
    n, tok = CHUNKS, local_rows // CHUNKS
    any_spec = pl.BlockSpec(memory_space=pl.ANY)
    vmem_spec = pl.BlockSpec(memory_space=pltpu.VMEM)
    vmem = pltpu.VMEM
    return pl.pallas_call(
        kernel,
        out_shape=jax.ShapeDtypeStruct((local_rows, width), BF16),
        in_specs=[any_spec, vmem_spec, any_spec, vmem_spec, any_spec, vmem_spec],
        out_specs=vmem_spec,
        scratch_shapes=[
            vmem((n, rows, tok, width), BF16),
            vmem((2 * feats, width), BF16),
            vmem((2, feats, width), BF16),
            vmem((2, 4, 2, 2, tok, 2 * feats), F32),
            vmem((n, 4, 2, tok, 2 * feats), F32),
            vmem((n, 2, tok, 2 * feats), BF16),
            vmem((n, 2, tok, 2 * feats), BF16),
            vmem((n, 2, tok, 2 * feats), F32),
            vmem((n, 2, tok, 2 * feats), F32),
            vmem((n, 2, tok, 2 * feats), BF16),
            vmem((n, 2, tok, 2 * feats), BF16),
            vmem((n, 2, tok, 2 * feats), BF16),
            vmem((n, 2, 4, tok, feats), BF16),
            vmem((n, 2, 2, 4, tok, width), BF16),
            vmem((n, rows, tok, width), BF16),
            vmem((128, 128), F32),
            pltpu.SemaphoreType.DMA((n + 5,)),
            pltpu.SemaphoreType.DMA((256,)),
            pltpu.SemaphoreType.DMA((176,)),
            pltpu.SemaphoreType.DMA((n, 16)),
        ],
        compiler_params=pltpu.CompilerParams(
            collective_id=0, has_side_effects=True, vmem_limit_bytes=63_000_000
        ),
        name="gated_ffn",
    )(
        act_quant, act_scale.reshape(8, 128),
        jnp.swapaxes(gate_up_quant, 1, 2).reshape(2 * feats, width), gate_up_scale,
        down_quant, down_scale.reshape(1, width),
    )


def solution(mesh):
    in_specs = (
        P("row", "col"),
        P(),
        P(None, "col", "row"),
        P(None, "row"),
        P("row", "col"),
        P("col"),
    )
    out_specs = P("row", "col")
    return jax.shard_map(body, mesh=mesh, in_specs=in_specs, out_specs=out_specs, check_vma=False)
```

```python
import jax
import jax.numpy as jnp
from jax import lax
from jax.experimental import pallas as pl
from jax.experimental.pallas import tpu as pltpu
from jax.sharding import PartitionSpec as P

MESH = pl.DeviceIdType.MESH
CHUNKS = 4
F32 = jnp.float32
BF16 = jnp.bfloat16
NEAR = (((0, 0), (0, 1)), ((0, 3), (1, 0)), ((3, 0), (1, 1)), ((3, 3), (1, 3)))
FAR = (((3, 1), (0, 2)), ((2, 0), (1, 2)), ((3, 2), (2, 1)), ((2, 3), (2, 2)))
PLACES = [(d, c, h) for h in range(2) for d in range(4) for c in range(2)]
PIECES = ((0, 1024, 0), (1024, 768, 0), (1792, 1024, 1), (2816, 880, 1))
GROUPS = ((0, (0,)), (0, (1,)), (1, (0, 1)), (2, (0, 1)), (3, (0, 1)))
UNITS = ((0, (0,)), (0, (1,)), (1, (1,)), (1, (0,)), (2, (1,)), (2, (0,)), (3, (1,)), (3, (0,)))
ORDER = (
    "A00 A10 A20 A30", "A01 B00 A11 B10", "B20 A21 B01 B30", "A31 B11 C00 C10", "B21 B31 C20 A02",
    "C30 C01 C11 C21", "A12 C31 B02 B03", "D.0 A22 A32 B12", "D.1 A03 B22 A13", "C02 B32 B13 C12",
    "E.0 B04 A23 B14", "C22 B23 C03 B05", "E.1 B33 A33 A04", "C13 B15 A14 A24", "B24 A34 B06 C32",
    "B25 B34 B16 C05", "C04 B26 C14 C23", "C33 B36 C24 C34", "D.2 F.1 B35 C06", "C16 C26 C36 D.4",
    "E.2 B07 F.0 C15", "C25 B17 D.6 E.4", "B27 C35 F.2 C07", "B37 C17 E.6 D.3", "F.4 C27 C37 J.0",
    "D.5 F.6 E.3 D.7", "E.5 F.3 E.7 F.5", "F.7 J.2 J.1 J.3",
)


def kernel(
    act_hbm, act_scale, gate_up_hbm, gate_up_scale, down_hbm, down_scale, out,
    act, w, dn, acc, pair, first, direct, merge, own, first_in, left_in, right_in,
    hid, o_send, o_recv, scale, load_sem, send_sem, recv_sem, out_sem,
    act_send, act_recv,
):
    n, tok, width = act.shape[0], act.shape[4], act.shape[5]
    half = width // 2
    feats = hid.shape[4]
    row, col = lax.axis_index("row"), lax.axis_index("col")
    z, y, x, core = row // 4, row % 4, col // 2, col % 2
    x1, x2, x3 = (x + 1) % 4, (x + 2) % 4, (x + 3) % 4
    xp, xm = (row, x1 * 2 + core), (row, x3 * 2 + core)
    mate = (row, x * 2 + 1 - core)

    def offset(d, c, h):
        return (NEAR, FAR)[h][d][c]

    def row_of(d, h, axis):
        own = (z, y)[axis]
        value = 0
        if isinstance(d, int):
            return (own + jnp.where(core == 0, *[offset(d, c, h)[axis] for c in range(2)])) % 4
        for k in range(4):
            pair_of = [offset(k, c, h)[axis] for c in range(2)]
            value = value + jnp.where(d == k, jnp.where(core == 0, *pair_of), 0)
        return (own + value) % 4

    def load(src, dst, index):
        copy = pltpu.make_async_copy(src, dst, load_sem.at[index])
        copy.start()
        return copy

    own_loads = [
        load(act_hbm.at[pl.ds(tok * i, tok)], act.at[i, 0, 0, 0], i) for i in range(n)
    ]
    w_loads = [
        load(gate_up_hbm.at[pl.ds(s, m)], w.at[pl.ds(s, m)], n + p)
        for p, (s, m, _) in enumerate(PIECES)
    ]
    dn_load = load(down_hbm, dn.at[core], n + len(PIECES))

    names, spare = {}, iter(range(149, 213))
    copies = {}

    def send(key, name, src, dst, device):
        index = names.setdefault((key, name), len(names))
        copy = pltpu.make_async_remote_copy(
            src_ref=src, dst_ref=dst, send_sem=send_sem.at[index],
            recv_sem=recv_sem.at[index],
            device_id=device, device_id_type=MESH,
        )
        copy.start()
        copies[key, name] = copy

    def got(key, *which):
        for name in which:
            copies[key, name].wait_recv()

    barrier = pltpu.get_barrier_semaphore()
    near = [xp, xm, mate] + [
        ((z + a) % 4 * 4 + (y + b) % 4, col) for a in range(4) for b in range(4) if a or b
    ]
    for device in near:
        pl.semaphore_signal(barrier, inc=1, device_id=device, device_id_type=MESH)

    lane = lax.broadcasted_iota(jnp.int32, (128, 128), 1)
    line = lax.broadcasted_iota(jnp.int32, (128, 128), 0)
    begins = []
    for h in range(2):
        source = row_of(x, h, 0) * 4 + row_of(x, h, 1)
        mine = jnp.broadcast_to(act_scale[pl.ds(source // 2, 1), :], (128, 128))
        column = jnp.sum(jnp.where(lane == line, mine, 0.0), axis=1, keepdims=True)
        scale[h] = jnp.broadcast_to(column, (128, 128))
        begins.append(source % 2 * 64)

    pl.semaphore_wait(barrier, len(near))

    def to_rows(i):
        for q, (d, c, h) in enumerate(PLACES[1:]):
            a, b = offset(d, c, h)
            yield h, pltpu.make_async_remote_copy(
                src_ref=act.at[i, 0, 0, 0], dst_ref=act.at[i, d, c, h],
                send_sem=act_send.at[i, q], recv_sem=act_recv.at[i, q],
                device_id=((z - a + 4) % 4 * 4 + (y - b + 4) % 4, col), device_id_type=MESH,
            )

    for i in range(n):
        own_loads[i].wait()
        for _, copy in to_rows(i):
            copy.start()
    send("dn", "", down_hbm, dn.at[core], mate)

    def stage_a(g, p):
        i, hs = GROUPS[g]
        start, size, _ = PIECES[p]
        cols, sl = pl.ds(start, size), pl.ds(hs[0], len(hs))
        if p == 0:
            for h, copy in to_rows(i):
                if h in hs:
                    copy.wait_recv()
            if g >= 2:
                for q in range(len(PIECES)):
                    copies.pop((("p", g - 2), q)).wait_send()
        if g == 0:
            w_loads[p].wait()
        part = lax.dot_general(
            act[i, :, :, sl].reshape(8 * len(hs) * tok, width), w[cols, :],
            (((1,), (1,)), ((), ())), preferred_element_type=F32,
        )
        s = g % 2
        acc[s, :, :, sl, :, cols] = part.reshape(4, 2, len(hs), tok, size)
        send(
            ("p", g), p, acc.at[s, :, 1 - core, sl, :, cols], pair.at[i, :, sl, :, cols], mate
        )

    paired = set()

    def slots(u):
        hs = UNITS[u][1]
        return pl.ds(hs[0], len(hs))

    def stage_b(u, p):
        i, hs = UNITS[u]
        start, size, side = PIECES[p]
        cols = pl.ds(start, size)
        g = [k for k, (c, rows) in enumerate(GROUPS) if c == i and hs[0] in rows][0]
        s, sl = g % 2, slots(u)

        def both(d):
            return acc[s, d, core, sl, :, cols] + pair[i, d, sl, :, cols]

        if (g, p) not in paired:
            paired.add((g, p))
            got(("p", g), p)
        near_dev, far_dev = (xm, xp) if side == 0 else (xp, xm)
        near_x, far_x = (x3, x1) if side == 0 else (x1, x3)
        landing = right_in if side == 0 else left_in
        first[i, sl, :, cols] = both(x2).astype(BF16)
        send(u, f"s{p}", first.at[i, sl, :, cols], first_in.at[i, sl, :, cols], far_dev)
        direct[i, sl, :, cols] = both(near_x).astype(BF16)
        send(u, f"d{p}", direct.at[i, sl, :, cols], landing.at[i, sl, :, cols], near_dev)
        merge[i, sl, :, cols] = both(far_x)
        own[i, sl, :, cols] = both(x)

    def stage_c(u, p):
        i, sl = UNITS[u][0], slots(u)
        start, size, side = PIECES[p]
        cols = pl.ds(start, size)
        far_dev, landing = (xp, left_in) if side == 0 else (xm, right_in)
        got(u, f"s{p}")
        copies.pop((u, f"s{p}")).wait_send()
        total = merge[i, sl, :, cols] + first_in[i, sl, :, cols].astype(F32)
        first[i, sl, :, cols] = total.astype(BF16)
        send(u, f"m{p}", first.at[i, sl, :, cols], landing.at[i, sl, :, cols], far_dev)

    def pass_on(u, name, d, device, start=0, size=None):
        i, sl = UNITS[u][0], slots(u)
        part = hid.at[i, sl, d, :, pl.ds(start, size or feats)]
        send(u, name, part, part, device)

    def stage_d(u):
        i, hs = UNITS[u]
        sl = slots(u)
        got(u, *[kind + str(p) for kind in "dm" for p in range(len(PIECES))])
        total = own[i, sl] + left_in[i, sl].astype(F32) + right_in[i, sl].astype(F32)
        total = total.reshape(len(hs) * tok, 2 * feats)
        token = jnp.concatenate(
            [scale[h, pl.ds(pl.multiple_of(begins[h] + tok * i, tok), tok), 0:1] for h in hs],
            axis=0,
        )
        gate = total[:, :feats] * token * gate_up_scale[0:1, :]
        up = total[:, feats:] * token * gate_up_scale[1:2, :]
        value = (gate / (1.0 + jnp.exp(-gate)) * up).astype(BF16)
        hid[i, sl, x] = value.reshape(len(hs), tok, feats)
        pass_on(u, "hp", x, xp)
        pass_on(u, "hm", x, xm)

    split = feats // 256 * 128

    def stage_e(u):
        got(u, "hp")
        pass_on(u, "hfp", x3, xp, 0, split)
        got(u, "hm")
        pass_on(u, "hfm", x1, xm, split, feats - split)

    def unless(skip, todo):
        if skip is None:
            todo()
        else:
            pl.when(jnp.logical_not(skip))(todo)

    out_sends = []

    def stage_f(u):
        i, hs = UNITS[u]
        sl = slots(u)
        got(u, "hfp", "hfm")
        if not out_sends:
            dn_load.wait()
            got("dn", "")
        count = len(hs)
        for h in range(2):
            for c in range(2):
                cols = pl.ds(c * half, half)
                part = jnp.dot(
                    hid[i, sl].reshape(count * 4 * tok, feats), dn[h, :, cols],
                    preferred_element_type=F32,
                )
                o_send[i, h, sl, :, :, cols] = part.astype(BF16).reshape(count, 4, tok, half)
            for slot in hs:
                for d in range(4):
                    device = (row_of(d, slot, 0) * 4 + row_of(d, slot, 1), x * 2 + h)
                    index = slot * 8 + d * 2 + core
                    skip = (core == 0) if (d, slot, h) == (0, 0, 0) else None

                    def build(h=h, slot=slot, d=d, device=device, index=index, k=next(spare)):
                        return pltpu.make_async_remote_copy(
                            src_ref=o_send.at[i, h, slot, d], dst_ref=o_recv.at[i, index],
                            send_sem=send_sem.at[k], recv_sem=out_sem.at[i, index],
                            device_id=device, device_id_type=MESH,
                        )

                    unless(skip, lambda build=build: build().start())
                    out_sends.append((skip, build))

    def stage_j(i):
        @pl.when(core == 0)
        def _():
            o_recv[i, 0] = o_send[i, 0, 0, 0]

        for q in range(16):
            def wait(q=q):
                pltpu.make_async_remote_copy(
                    src_ref=o_recv.at[i, q], dst_ref=o_recv.at[i, q],
                    send_sem=send_sem.at[0], recv_sem=out_sem.at[i, q],
                    device_id=mate, device_id_type=MESH,
                ).wait_recv()

            unless(core == 0 if q == 0 else None, wait)
        total = o_recv[i, 0].astype(F32)
        for q in range(1, 16):
            total = total + o_recv[i, q].astype(F32)
        out[pl.ds(tok * i, tok), :] = (total * down_scale[...]).astype(BF16)

    stages = {
        "A": stage_a, "B": stage_b, "C": stage_c, "D": stage_d,
        "E": stage_e, "F": stage_f, "J": stage_j,
    }
    for words in ORDER:
        for word in words.split():
            name, piece, chunk = word
            if piece == ".":
                stages[name](int(chunk))
            else:
                stages[name](int(chunk), int(piece))
    for copy in copies.values():
        copy.wait_send()
    for i in range(n):
        for _, copy in to_rows(i):
            copy.wait_send()
    for skip, build in out_sends:
        unless(skip, lambda build=build: build().wait_send())


def body(act_quant, act_scale, gate_up_quant, gate_up_scale, down_quant, down_scale):
    local_rows, width = act_quant.shape
    feats = gate_up_quant.shape[2]
    rows = lax.axis_size("row")
    n, tok = CHUNKS, local_rows // CHUNKS
    any_spec = pl.BlockSpec(memory_space=pl.ANY)
    vmem_spec = pl.BlockSpec(memory_space=pltpu.VMEM)
    vmem = pltpu.VMEM
    return pl.pallas_call(
        kernel,
        out_shape=jax.ShapeDtypeStruct((local_rows, width), BF16),
        in_specs=[any_spec, vmem_spec, any_spec, vmem_spec, any_spec, vmem_spec],
        out_specs=vmem_spec,
        scratch_shapes=[
            vmem((n, 4, 2, 2, tok, width), BF16),
            vmem((2 * feats, width), BF16),
            vmem((2, feats, width), BF16),
            vmem((2, 4, 2, 2, tok, 2 * feats), F32),
            vmem((n, 4, 2, tok, 2 * feats), F32),
            vmem((n, 2, tok, 2 * feats), BF16),
            vmem((n, 2, tok, 2 * feats), BF16),
            vmem((n, 2, tok, 2 * feats), F32),
            vmem((n, 2, tok, 2 * feats), F32),
            vmem((n, 2, tok, 2 * feats), BF16),
            vmem((n, 2, tok, 2 * feats), BF16),
            vmem((n, 2, tok, 2 * feats), BF16),
            vmem((n, 2, 4, tok, feats), BF16),
            vmem((n, 2, 2, 4, tok, width), BF16),
            vmem((n, rows, tok, width), BF16),
            vmem((2, 128, 128), F32),
            pltpu.SemaphoreType.DMA((n + 5,)),
            pltpu.SemaphoreType.DMA((213,)),
            pltpu.SemaphoreType.DMA((149,)),
            pltpu.SemaphoreType.DMA((n, 16)),
            pltpu.SemaphoreType.DMA((n, 15)),
            pltpu.SemaphoreType.DMA((n, 15)),
        ],
        compiler_params=pltpu.CompilerParams(
            collective_id=0, has_side_effects=True, vmem_limit_bytes=63_000_000
        ),
        name="gated_ffn",
    )(
        act_quant, act_scale.reshape(8, 128),
        jnp.swapaxes(gate_up_quant, 1, 2).reshape(2 * feats, width), gate_up_scale,
        down_quant, down_scale.reshape(1, width),
    )


def solution(mesh):
    in_specs = (
        P("row", "col"),
        P(),
        P(None, "col", "row"),
        P(None, "row"),
        P("row", "col"),
        P("col"),
    )
    out_specs = P("row", "col")
    return jax.shard_map(body, mesh=mesh, in_specs=in_specs, out_specs=out_specs, check_vma=False)
```

```python
import jax
import jax.numpy as jnp
from jax import lax
from jax.experimental import pallas as pl
from jax.experimental.pallas import tpu as pltpu
from jax.sharding import PartitionSpec as P

MESH = pl.DeviceIdType.MESH
CHUNKS = 4
F32 = jnp.float32
BF16 = jnp.bfloat16
NEAR = (((0, 0), (0, 1)), ((0, 3), (1, 0)), ((3, 0), (1, 1)), ((3, 3), (1, 3)))
FAR = (((3, 1), (0, 2)), ((2, 0), (1, 2)), ((3, 2), (2, 1)), ((2, 3), (2, 2)))
PLACES = [(d, c, h) for h in range(2) for d in range(4) for c in range(2)]
PIECES = ((0, 1024, 0), (1024, 768, 0), (1792, 1024, 1), (2816, 880, 1))
GROUPS = ((0, (0,)), (0, (1,)), (1, (0, 1)), (2, (0, 1)), (3, (0, 1)))
UNITS = ((0, (0,)), (0, (1,)), (1, (1,)), (1, (0,)), (2, (1,)), (2, (0,)), (3, (1,)), (3, (0,)))
ORDER = (
    "A00 A10 A20 A30", "A01 B00 A11 B10", "B20 A21 B01 B30", "A31 B11 C00 C10", "B21 B31 C20 A02",
    "C30 C01 C11 C21", "A12 C31 B02 B03", "D.0 A22 A32 B12", "D.1 A03 B22 A13", "C02 B32 B13 C12",
    "E.0 B04 A23 B14", "C22 B23 C03 B05", "E.1 B33 A33 A04", "C13 B15 A14 A24", "B24 A34 B06 C32",
    "B25 B34 B16 C05", "C04 B26 C14 C23", "C33 B36 C24 C34", "D.2 F.1 B35 C06", "C16 C26 C36 D.4",
    "E.2 B07 F.0 C15", "C25 B17 D.6 E.4", "B27 C35 F.2 C07", "B37 C17 E.6 D.3", "F.4 C27 C37 J.0",
    "D.5 F.6 E.3 D.7", "E.5 F.3 E.7 F.5", "F.7 J.2 J.1 J.3",
)


def kernel(
    act_hbm, act_scale, gate_up_hbm, gate_up_scale, down_hbm, down_scale, out,
    act, w, dn, acc, pair, first, direct, merge, own, first_in, left_in, right_in,
    hid, o_send, o_recv, scale, load_sem, send_sem, recv_sem, out_sem,
    act_send, act_recv,
):
    n, tok, width = act.shape[0], act.shape[4], act.shape[5]
    half = width // 2
    feats = hid.shape[4]
    row, col = lax.axis_index("row"), lax.axis_index("col")
    z, y, x, core = row // 4, row % 4, col // 2, col % 2
    x1, x2, x3 = (x + 1) % 4, (x + 2) % 4, (x + 3) % 4
    xp, xm = (row, x1 * 2 + core), (row, x3 * 2 + core)
    mate = (row, x * 2 + 1 - core)

    def offset(d, c, h):
        return (NEAR, FAR)[h][d][c]

    def row_of(d, h, axis):
        own = (z, y)[axis]
        value = 0
        if isinstance(d, int):
            return (own + jnp.where(core == 0, *[offset(d, c, h)[axis] for c in range(2)])) % 4
        for k in range(4):
            pair_of = [offset(k, c, h)[axis] for c in range(2)]
            value = value + jnp.where(d == k, jnp.where(core == 0, *pair_of), 0)
        return (own + value) % 4

    def load(src, dst, index):
        copy = pltpu.make_async_copy(src, dst, load_sem.at[index])
        copy.start()
        return copy

    own_loads = [
        load(act_hbm.at[pl.ds(tok * i, tok)], act.at[i, 0, 0, 0], i) for i in range(n)
    ]
    w_loads = [
        load(gate_up_hbm.at[pl.ds(s, m)], w.at[pl.ds(s, m)], n + p)
        for p, (s, m, _) in enumerate(PIECES)
    ]
    dn_load = load(down_hbm, dn.at[core], n + len(PIECES))

    names, spare = {}, iter(range(149, 213))
    copies = {}

    def send(key, name, src, dst, device):
        index = names.setdefault((key, name), len(names))
        copy = pltpu.make_async_remote_copy(
            src_ref=src, dst_ref=dst, send_sem=send_sem.at[index],
            recv_sem=recv_sem.at[index],
            device_id=device, device_id_type=MESH,
        )
        copy.start()
        copies[key, name] = copy

    def got(key, *which):
        for name in which:
            copies[key, name].wait_recv()

    barrier = pltpu.get_barrier_semaphore()
    near = [xp, xm, mate] + [
        ((z + a) % 4 * 4 + (y + b) % 4, col) for a in range(4) for b in range(4) if a or b
    ]
    for device in near:
        pl.semaphore_signal(barrier, inc=1, device_id=device, device_id_type=MESH)

    lane = lax.broadcasted_iota(jnp.int32, (128, 128), 1)
    line = lax.broadcasted_iota(jnp.int32, (128, 128), 0)
    begins = []
    for h in range(2):
        source = row_of(x, h, 0) * 4 + row_of(x, h, 1)
        mine = jnp.broadcast_to(act_scale[pl.ds(source // 2, 1), :], (128, 128))
        column = jnp.sum(jnp.where(lane == line, mine, 0.0), axis=1, keepdims=True)
        scale[h] = jnp.broadcast_to(column, (128, 128))
        begins.append(source % 2 * 64)

    pl.semaphore_wait(barrier, len(near))

    def to_rows(i):
        for q, (d, c, h) in enumerate(PLACES[1:]):
            a, b = offset(d, c, h)
            yield h, pltpu.make_async_remote_copy(
                src_ref=act.at[i, 0, 0, 0], dst_ref=act.at[i, d, c, h],
                send_sem=act_send.at[i, q], recv_sem=act_recv.at[i, q],
                device_id=((z - a + 4) % 4 * 4 + (y - b + 4) % 4, col), device_id_type=MESH,
            )

    for i in range(n):
        own_loads[i].wait()
        for _, copy in to_rows(i):
            copy.start()
    send("dn", "", down_hbm, dn.at[core], mate)

    def stage_a(g, p):
        i, hs = GROUPS[g]
        start, size, _ = PIECES[p]
        cols, sl = pl.ds(start, size), pl.ds(hs[0], len(hs))
        if p == 0:
            for h, copy in to_rows(i):
                if h in hs:
                    copy.wait_recv()
            if g >= 2:
                for q in range(len(PIECES)):
                    copies.pop((("p", g - 2), q)).wait_send()
        if g == 0:
            w_loads[p].wait()
        part = lax.dot_general(
            act[i, :, :, sl].reshape(8 * len(hs) * tok, width), w[cols, :],
            (((1,), (1,)), ((), ())), preferred_element_type=F32,
        )
        s = g % 2
        acc[s, :, :, sl, :, cols] = part.reshape(4, 2, len(hs), tok, size)
        send(
            ("p", g), p, acc.at[s, :, 1 - core, sl, :, cols], pair.at[i, :, sl, :, cols], mate
        )

    paired = set()

    def slots(u):
        hs = UNITS[u][1]
        return pl.ds(hs[0], len(hs))

    def stage_b(u, p):
        i, hs = UNITS[u]
        start, size, side = PIECES[p]
        cols = pl.ds(start, size)
        g = [k for k, (c, rows) in enumerate(GROUPS) if c == i and hs[0] in rows][0]
        s, sl = g % 2, slots(u)

        def both(d):
            return acc[s, d, core, sl, :, cols] + pair[i, d, sl, :, cols]

        if (g, p) not in paired:
            paired.add((g, p))
            got(("p", g), p)
        near_dev, far_dev = (xm, xp) if side == 0 else (xp, xm)
        near_x, far_x = (x3, x1) if side == 0 else (x1, x3)
        landing = right_in if side == 0 else left_in
        first[i, sl, :, cols] = both(x2).astype(BF16)
        send(u, f"s{p}", first.at[i, sl, :, cols], first_in.at[i, sl, :, cols], far_dev)
        direct[i, sl, :, cols] = both(near_x).astype(BF16)
        send(u, f"d{p}", direct.at[i, sl, :, cols], landing.at[i, sl, :, cols], near_dev)
        merge[i, sl, :, cols] = both(far_x)
        own[i, sl, :, cols] = both(x)

    def stage_c(u, p):
        i, sl = UNITS[u][0], slots(u)
        start, size, side = PIECES[p]
        cols = pl.ds(start, size)
        far_dev, landing = (xp, left_in) if side == 0 else (xm, right_in)
        got(u, f"s{p}")
        copies.pop((u, f"s{p}")).wait_send()
        total = merge[i, sl, :, cols] + first_in[i, sl, :, cols].astype(F32)
        first[i, sl, :, cols] = total.astype(BF16)
        send(u, f"m{p}", first.at[i, sl, :, cols], landing.at[i, sl, :, cols], far_dev)

    def pass_on(u, name, d, device, start=0, size=None):
        i, sl = UNITS[u][0], slots(u)
        part = hid.at[i, sl, d, :, pl.ds(start, size or feats)]
        send(u, name, part, part, device)

    def stage_d(u):
        i, hs = UNITS[u]
        sl = slots(u)
        got(u, *[kind + str(p) for kind in "dm" for p in range(len(PIECES))])
        total = own[i, sl] + left_in[i, sl].astype(F32) + right_in[i, sl].astype(F32)
        total = total.reshape(len(hs) * tok, 2 * feats)
        token = jnp.concatenate(
            [scale[h, pl.ds(pl.multiple_of(begins[h] + tok * i, tok), tok), 0:1] for h in hs],
            axis=0,
        )
        gate = total[:, :feats] * token * gate_up_scale[0:1, :]
        up = total[:, feats:] * token * gate_up_scale[1:2, :]
        value = (gate / (1.0 + jnp.exp(-gate)) * up).astype(BF16)
        hid[i, sl, x] = value.reshape(len(hs), tok, feats)
        pass_on(u, "hp", x, xp)
        pass_on(u, "hm", x, xm)

    split = feats // 256 * 128

    def stage_e(u):
        got(u, "hp")
        pass_on(u, "hfp", x3, xp, 0, split)
        got(u, "hm")
        pass_on(u, "hfm", x1, xm, split, feats - split)

    def unless(skip, todo):
        if skip is None:
            todo()
        else:
            pl.when(jnp.logical_not(skip))(todo)

    out_sends = []

    def stage_f(u):
        i, hs = UNITS[u]
        sl = slots(u)
        got(u, "hfp", "hfm")
        if not out_sends:
            dn_load.wait()
            got("dn", "")
        count = len(hs)
        for h in range(2):
            for c in range(2):
                cols = pl.ds(c * half, half)
                part = jnp.dot(
                    hid[i, sl].reshape(count * 4 * tok, feats), dn[h, :, cols],
                    preferred_element_type=F32,
                )
                o_send[i, h, sl, :, :, cols] = part.astype(BF16).reshape(count, 4, tok, half)
            for slot in hs:
                for d in range(4):
                    device = (row_of(d, slot, 0) * 4 + row_of(d, slot, 1), x * 2 + h)
                    index = slot * 8 + d * 2 + core
                    skip = (core == 0) if (d, slot, h) == (0, 0, 0) else None

                    def build(h=h, slot=slot, d=d, device=device, index=index, k=next(spare)):
                        return pltpu.make_async_remote_copy(
                            src_ref=o_send.at[i, h, slot, d], dst_ref=o_recv.at[i, index],
                            send_sem=send_sem.at[k], recv_sem=out_sem.at[i, index],
                            device_id=device, device_id_type=MESH,
                        )

                    unless(skip, lambda build=build: build().start())
                    out_sends.append((skip, build))

    def stage_j(i):
        @pl.when(core == 0)
        def _():
            o_recv[i, 0] = o_send[i, 0, 0, 0]

        for q in range(16):
            def wait(q=q):
                pltpu.make_async_remote_copy(
                    src_ref=o_recv.at[i, q], dst_ref=o_recv.at[i, q],
                    send_sem=send_sem.at[0], recv_sem=out_sem.at[i, q],
                    device_id=mate, device_id_type=MESH,
                ).wait_recv()

            unless(core == 0 if q == 0 else None, wait)
        total = o_recv[i, 0].astype(F32)
        for q in range(1, 16):
            total = total + o_recv[i, q].astype(F32)
        out[pl.ds(tok * i, tok), :] = (total * down_scale[...]).astype(BF16)

    stages = {
        "A": stage_a, "B": stage_b, "C": stage_c, "D": stage_d,
        "E": stage_e, "F": stage_f, "J": stage_j,
    }
    words = " ".join(ORDER).split()
    early = 0
    for at, word in enumerate(words):
        name, piece, chunk = word
        if at == len(words) - 1:
            for copy in copies.values():
                copy.wait_send()
            for i in range(n):
                for _, copy in to_rows(i):
                    copy.wait_send()
            early = len(out_sends) - 24
            for skip, build in out_sends[:early]:
                unless(skip, lambda build=build: build().wait_send())
        if piece == ".":
            stages[name](int(chunk))
        else:
            stages[name](int(chunk), int(piece))
    for skip, build in out_sends[early:]:
        unless(skip, lambda build=build: build().wait_send())


def body(act_quant, act_scale, gate_up_quant, gate_up_scale, down_quant, down_scale):
    local_rows, width = act_quant.shape
    feats = gate_up_quant.shape[2]
    rows = lax.axis_size("row")
    n, tok = CHUNKS, local_rows // CHUNKS
    any_spec = pl.BlockSpec(memory_space=pl.ANY)
    vmem_spec = pl.BlockSpec(memory_space=pltpu.VMEM)
    vmem = pltpu.VMEM
    return pl.pallas_call(
        kernel,
        out_shape=jax.ShapeDtypeStruct((local_rows, width), BF16),
        in_specs=[any_spec, vmem_spec, any_spec, vmem_spec, any_spec, vmem_spec],
        out_specs=vmem_spec,
        scratch_shapes=[
            vmem((n, 4, 2, 2, tok, width), BF16),
            vmem((2 * feats, width), BF16),
            vmem((2, feats, width), BF16),
            vmem((2, 4, 2, 2, tok, 2 * feats), F32),
            vmem((n, 4, 2, tok, 2 * feats), F32),
            vmem((n, 2, tok, 2 * feats), BF16),
            vmem((n, 2, tok, 2 * feats), BF16),
            vmem((n, 2, tok, 2 * feats), F32),
            vmem((n, 2, tok, 2 * feats), F32),
            vmem((n, 2, tok, 2 * feats), BF16),
            vmem((n, 2, tok, 2 * feats), BF16),
            vmem((n, 2, tok, 2 * feats), BF16),
            vmem((n, 2, 4, tok, feats), BF16),
            vmem((n, 2, 2, 4, tok, width), BF16),
            vmem((n, rows, tok, width), BF16),
            vmem((2, 128, 128), F32),
            pltpu.SemaphoreType.DMA((n + 5,)),
            pltpu.SemaphoreType.DMA((213,)),
            pltpu.SemaphoreType.DMA((149,)),
            pltpu.SemaphoreType.DMA((n, 16)),
            pltpu.SemaphoreType.DMA((n, 15)),
            pltpu.SemaphoreType.DMA((n, 15)),
        ],
        compiler_params=pltpu.CompilerParams(
            collective_id=0, has_side_effects=True, vmem_limit_bytes=63_000_000
        ),
        name="gated_ffn",
    )(
        act_quant, act_scale.reshape(8, 128),
        jnp.swapaxes(gate_up_quant, 1, 2).reshape(2 * feats, width), gate_up_scale,
        down_quant, down_scale.reshape(1, width),
    )


def solution(mesh):
    in_specs = (
        P("row", "col"),
        P(),
        P(None, "col", "row"),
        P(None, "row"),
        P("row", "col"),
        P("col"),
    )
    out_specs = P("row", "col")
    return jax.shard_map(body, mesh=mesh, in_specs=in_specs, out_specs=out_specs, check_vma=False)
```
